32 devices in a mesh: groups: 2 (over x), col: 16 (over z, y, core).
Axes of the slice: x: 2, y: 2, z: 4, core: 2. Of those that a mesh axis runs over, the one named last changes fastest.
Arguments:
- left: bfloat16 [256, 64, 32], P('col', 'groups'), parts along dimension 1, may hold values from -18 to 18
- right: bfloat16 [256, 2560, 32], P('col', 'groups'), parts along dimension 1, may hold values from -18 to 18
- out_weight: bfloat16 [1024, 128], replicated, may hold values from -0.1875 to 0.1875
- out_bias: float32 [128], replicated, may hold values from -3 to 3
Outputs:
- pair_update: bfloat16 [64, 1280, 128], P('groups', 'col'), parts along dimension 0
The draws below stay inside these ranges and needn't reach their ends.
There are 2 independent parts, one for each index of `groups`. The reference program is written for one: setup_inputs(seed, part) draws one part's arguments, and reference() takes and returns one part's arrays. A program takes and returns all parts, laid end to end along the dimension named above; an argument that names none is the same for every part. Nothing has to cross between parts.
All inputs are finite; a program needn't handle non-finite values.
Results may differ from the reference program's by a relative error of at most 0.004.
Values may be sent and summed in bfloat16 or wider, within the bound.
A program may use at most 64 MiB of HBM per device.

```python
import jax
import jax.numpy as jnp
from jax import lax

C = 32
PAIR = 128
S = 256
COL_DEV = 80
R = 1280
ROWS = 32
CC = 1024
N_COL = 16


def levels(own_key, dims, split, low, largest):
    def one(dim, shards_of):
        heights = jax.random.uniform(jax.random.fold_in(jax.random.fold_in(own_key, 6), dim), (shards_of,), jnp.float32, low / len(split), largest / len(split))
        return jnp.repeat(jnp.exp(heights), dims[dim] // shards_of).reshape((-1,) + (1,) * (len(dims) - dim - 1))

    loudness = one(*split[0])
    for cut in split[1:]:
        loudness = loudness * one(*cut)
    return loudness


def bell_draw(rng, shape, deviation, limit, split=(), kind=jnp.bfloat16):
    level = levels(rng, shape, split, -0.22, 0.18) if split else 1.0
    result = jax.random.normal(rng, shape, jnp.float32) * deviation * level
    return jnp.minimum(jnp.maximum(result, -limit), limit).astype(kind)


def setup_inputs(seed: int = 0, part: int = 0) -> dict:
    key_list = jax.random.split(jax.random.key(seed), 5)
    part_keys = jax.random.split(jax.random.fold_in(key_list[4], part), 5)
    left = bell_draw(part_keys[0], (S, ROWS, C), 3.0, 18.0, ((0, 16),))
    right = bell_draw(part_keys[1], (S, R, C), 3.0, 18.0, ((0, 16),))
    out_weight = bell_draw(key_list[2], (CC, PAIR), CC ** -0.5, 0.1875)
    out_bias = bell_draw(key_list[3], (PAIR,), 0.5, 3.0, (), jnp.float32)
    return {"left": left, "right": right, "out_weight": out_weight, "out_bias": out_bias}


def reference(left, right, out_weight, out_bias):
    left_wide = left.astype(jnp.float32)
    right_wide = right.astype(jnp.float32)

    def column_block(index):
        start = (index * COL_DEV).astype(jnp.int32)
        block = lax.dynamic_slice_in_dim(right_wide, start, COL_DEV, 1)
        outer = jnp.einsum("sic,sje->ijce", left_wide, block, precision=lax.Precision.HIGHEST) / S
        flat = outer.astype(jnp.bfloat16).reshape(ROWS * COL_DEV, C * C)
        update = jnp.dot(flat, out_weight, preferred_element_type=jnp.float32) + out_bias
        return update.astype(jnp.bfloat16).reshape(ROWS, COL_DEV, PAIR)

    blocks = lax.map(column_block, jnp.arange(N_COL, dtype=jnp.int32))
    return jnp.transpose(blocks, (1, 0, 2, 3)).reshape(ROWS, N_COL * COL_DEV, PAIR)
```

```python
import functools

import jax
import jax.numpy as jnp
from jax import lax
from jax.experimental import pallas as pl
from jax.experimental.pallas import tpu as pltpu
from jax.sharding import PartitionSpec as P

MESH = pl.DeviceIdType.MESH
LANES = 128
TILE = 16


def flip_kernel(x_ref, o_ref):
    o_ref[...] = x_ref[...].T


def flip(x):
    rows, columns = x.shape
    step = 2 * LANES
    return pl.pallas_call(
        flip_kernel,
        grid=(columns // step,),
        in_specs=[pl.BlockSpec((rows, step), lambda g: (0, g))],
        out_specs=pl.BlockSpec((step, rows), lambda g: (g, 0)),
        out_shape=jax.ShapeDtypeStruct((columns, rows), x.dtype),
    )(x)


def swap_matrix(first, minor, start, rows, columns):
    row = lax.broadcasted_iota(jnp.int32, (rows, columns), 0) + start
    column = lax.broadcasted_iota(jnp.int32, (rows, columns), 1)
    shift = first.bit_length() - 1
    wanted = (row & (first - 1)) * minor + (row >> shift)
    return jnp.where(column == wanted, 1.0, 0.0).astype(jnp.bfloat16)


def kernel(
    n, width, cols, rows, right_ref, left_ref, weight_ref, bias_ref, out_ref,
    rbuf, lbuf, rwide, lturn, wturn, flat,
    rsend, rrecv, lsend, lrecv, fsend, own,
):
    me = lax.axis_index("col")
    mate = me + 1 - 2 * lax.rem(me, 2)
    half = n // 2
    pair = out_ref.shape[2]
    local = left_ref.shape[0]
    seqs = n * local

    def rcopy(k):
        to = lax.rem(me + k, n)
        start = pl.multiple_of(to * cols, TILE)
        return pltpu.make_async_remote_copy(
            src_ref=right_ref.at[pl.ds(start, cols)],
            dst_ref=rbuf.at[me],
            send_sem=rsend.at[k],
            recv_sem=rrecv.at[me],
            device_id={"col": to},
            device_id_type=MESH,
        )

    def lcopy(src, slot, to, send):
        return pltpu.make_async_remote_copy(
            src_ref=src,
            dst_ref=lbuf.at[slot],
            send_sem=send,
            recv_sem=lrecv.at[slot],
            device_id={"col": to},
            device_id_type=MESH,
        )

    barrier = pltpu.get_barrier_semaphore()
    for k in range(1, n):
        pl.semaphore_signal(
            barrier, inc=1, device_id={"col": lax.rem(me + k, n)}, device_id_type=MESH
        )
    pl.semaphore_wait(barrier, n - 1)

    sends = [lcopy(left_ref, me, mate, lsend.at[0])]
    for k in range(1, half):
        sends.append(lcopy(left_ref, me, lax.rem(me + 2 * k, n), lsend.at[k]))
    for k in range(1, n):
        sends.append(rcopy(k))
    for copy in sends:
        copy.start()
    mine = pltpu.make_async_copy(
        right_ref.at[pl.ds(pl.multiple_of(me * cols, TILE), cols)], rbuf.at[me], own.at[0]
    )
    mine.start()
    mine_left = pltpu.make_async_copy(left_ref, lbuf.at[me], own.at[1])
    mine_left.start()

    rwide[...] = jnp.zeros_like(rwide)
    channels = width * width
    for start in range(0, channels, LANES):
        chosen = swap_matrix(width, width, start, LANES, channels)
        block = jnp.dot(chosen, weight_ref[...], preferred_element_type=jnp.float32)
        wturn[:, start : start + LANES] = block.T.astype(jnp.bfloat16)
    swap = swap_matrix(TILE, width, 0, TILE * width, TILE * width)

    forwards = []
    for k in range(1, half):
        slot = lax.rem(me + n - 2 * k, n)
        lcopy(left_ref, slot, mate, lsend.at[k]).wait_recv()
        forward = lcopy(lbuf.at[slot], slot, mate, fsend.at[k])
        forward.start()
        forwards.append(forward)
    lcopy(left_ref, mate, mate, lsend.at[0]).wait_recv()
    for k in range(1, half):
        slot = lax.rem(mate + n - 2 * k, n)
        lcopy(left_ref, slot, mate, lsend.at[k]).wait_recv()
    mine_left.wait()
    per = TILE // local
    for group in range(seqs // TILE):
        parts = [lbuf[group * per + p] for p in range(per)]
        if per > 1:
            parts = [part.astype(jnp.float32) for part in parts]
            block = jnp.concatenate(parts, axis=0).astype(jnp.bfloat16)
        else:
            block = parts[0]
        lturn[group * TILE : (group + 1) * TILE, :] = block

    mine.wait()
    for k in range(1, n):
        slot = lax.rem(me + n - k, n)
        pltpu.make_async_remote_copy(
            src_ref=right_ref.at[pl.ds(0, cols)],
            dst_ref=rbuf.at[slot],
            send_sem=rsend.at[k],
            recv_sem=rrecv.at[slot],
            device_id={"col": slot},
            device_id_type=MESH,
        ).wait_recv()
    for group in range(seqs // TILE):
        parts = [rbuf[group * per + p] for p in range(per)]
        block = parts[0] if per == 1 else jnp.concatenate(parts, axis=1)
        turned = lax.dot_general(
            swap, block, (((1,), (1,)), ((), ())), preferred_element_type=jnp.float32
        ).astype(jnp.bfloat16)
        for e in range(width):
            rwide[group * TILE : (group + 1) * TILE, e * LANES : e * LANES + cols] = turned[
                e * TILE : (e + 1) * TILE
            ]

    count = flat.shape[0] * 2
    for base in range(0, rows, count):
        turned = lturn[:, base * width : (base + count) * width].T

        def outer(step, carry):
            lanes = pl.ds(pl.multiple_of(step * 2 * LANES, 2 * LANES), 2 * LANES)
            product = jnp.dot(
                turned, rwide[:, lanes], preferred_element_type=jnp.float32
            ).astype(jnp.bfloat16)
            for half_e in range(2):
                at = pl.ds(pl.multiple_of((step * 2 + half_e) * width, width), width)
                for i in range(count):
                    side = (i % 2) * LANES
                    flat[i // 2, at, side : side + LANES] = product[
                        i * width : (i + 1) * width, half_e * LANES : (half_e + 1) * LANES
                    ]
            return carry

        lax.fori_loop(0, width // 2, outer, 0)

        def project(step, carry):
            update = jnp.dot(wturn[...], flat[step], preferred_element_type=jnp.float32).T
            update = update * (1.0 / seqs) + bias_ref[...]
            update = update.astype(out_ref.dtype)
            out_ref[base + 2 * step] = update[:cols]
            out_ref[base + 2 * step + 1] = update[LANES : LANES + cols]
            return carry

        lax.fori_loop(0, count // 2, project, 0)

    for copy in sends + forwards:
        copy.wait_send()


def on_device(n, left, right, out_weight, out_bias):
    local, rows, width = left.shape
    cols = right.shape[1] // n
    pair = out_weight.shape[1]
    seqs = local * n
    wide = jnp.transpose(right, (0, 2, 1)).reshape(local * width, right.shape[1])
    turned = flip(wide)
    rows_step = min(rows, 32)
    vmem = pl.BlockSpec(memory_space=pltpu.VMEM)
    dma = pltpu.SemaphoreType.DMA
    return pl.pallas_call(
        functools.partial(kernel, n, width, cols, rows),
        out_shape=jax.ShapeDtypeStruct((rows, cols, pair), jnp.bfloat16),
        in_specs=[vmem] * 4,
        out_specs=vmem,
        scratch_shapes=[
            pltpu.VMEM((n, cols, local * width), jnp.bfloat16),
            pltpu.VMEM((n, local, rows * width), jnp.bfloat16),
            pltpu.VMEM((seqs, width * LANES), jnp.bfloat16),
            pltpu.VMEM((seqs, rows * width), jnp.bfloat16),
            pltpu.VMEM((pair, width * width), jnp.bfloat16),
            pltpu.VMEM((rows_step // 2, width * width, 2 * LANES), jnp.bfloat16),
            dma((n,)), dma((n,)), dma((n // 2,)), dma((n,)), dma((n // 2,)), dma((2,)),
        ],
        compiler_params=pltpu.CompilerParams(
            collective_id=0, has_side_effects=True, vmem_limit_bytes=60 * 1024 * 1024
        ),
    )(turned, left.reshape(local, rows * width), out_weight, out_bias.reshape(1, pair))


def solution(mesh):
    return jax.shard_map(
        functools.partial(on_device, mesh.shape["col"]),
        mesh=mesh,
        in_specs=(P("col", "groups", None), P("col", "groups", None), P(), P()),
        out_specs=P("groups", "col", None),
        check_vma=False,
    )
```

```python
import functools

import jax
import jax.numpy as jnp
from jax import lax
from jax.experimental import pallas as pl
from jax.experimental.pallas import tpu as pltpu
from jax.sharding import PartitionSpec as P

MESH = pl.DeviceIdType.MESH
LANES = 128
TILE = 16
GROUP = 4


def flip_kernel(x_ref, o_ref):
    chunks, _, lanes = o_ref.shape
    local, width, step = x_ref.shape
    part = width // chunks
    for h in range(chunks):
        piece = x_ref[:, h * part : (h + 1) * part, :]
        o_ref[h] = piece.reshape(lanes, step).T


def flip(x, chunks):
    local, width, columns = x.shape
    step = 2 * LANES
    lanes = local * width // chunks
    return pl.pallas_call(
        flip_kernel,
        grid=(columns // step,),
        in_specs=[pl.BlockSpec((local, width, step), lambda g: (0, 0, g))],
        out_specs=pl.BlockSpec((chunks, step, lanes), lambda g: (0, g, 0)),
        out_shape=jax.ShapeDtypeStruct((chunks, columns, lanes), x.dtype),
    )(x)


def swap_matrix(first, minor, start, rows, columns):
    row = lax.broadcasted_iota(jnp.int32, (rows, columns), 0) + start
    column = lax.broadcasted_iota(jnp.int32, (rows, columns), 1)
    shift = first.bit_length() - 1
    wanted = (row & (first - 1)) * minor + (row >> shift)
    return jnp.where(column == wanted, 1.0, 0.0).astype(jnp.bfloat16)


def kernel(
    n, width, cols, rows, chunks, right_ref, left_ref, weight_ref, bias_ref, out_ref,
    rbuf, lbuf, rwide, lturn, wturn, flat, partial,
    rsend, rrecv, lsend, lrecv, fsend, own,
):
    me = lax.axis_index("col")
    place = lax.rem(me, GROUP)
    mates = [me - place + lax.rem(place + j, GROUP) for j in range(1, GROUP)]
    hops = n // GROUP
    local = left_ref.shape[0]
    seqs = n * local
    part = width // chunks

    def rcopy(h, k):
        to = lax.rem(me + k, n)
        start = pl.multiple_of(to * cols, TILE)
        return pltpu.make_async_remote_copy(
            src_ref=right_ref.at[h, pl.ds(start, cols)],
            dst_ref=rbuf.at[h, me],
            send_sem=rsend.at[h, k],
            recv_sem=rrecv.at[h, me],
            device_id={"col": to},
            device_id_type=MESH,
        )

    def lcopy(src, slot, to, send):
        return pltpu.make_async_remote_copy(
            src_ref=src,
            dst_ref=lbuf.at[slot],
            send_sem=send,
            recv_sem=lrecv.at[slot],
            device_id={"col": to},
            device_id_type=MESH,
        )

    barrier = pltpu.get_barrier_semaphore()
    for k in range(1, n):
        pl.semaphore_signal(
            barrier, inc=1, device_id={"col": lax.rem(me + k, n)}, device_id_type=MESH
        )
    pl.semaphore_wait(barrier, n - 1)

    sends = []
    for k in range(1, hops):
        sends.append(lcopy(left_ref, me, lax.rem(me + GROUP * k, n), lsend.at[k]))
    for j, mate in enumerate(mates):
        sends.append(lcopy(left_ref, me, mate, fsend.at[0, j]))
    for h in range(chunks):
        for k in range(1, n):
            sends.append(rcopy(h, k))
    for copy in sends:
        copy.start()
    mine = []
    for h in range(chunks):
        block = right_ref.at[h, pl.ds(pl.multiple_of(me * cols, TILE), cols)]
        mine.append(pltpu.make_async_copy(block, rbuf.at[h, me], own.at[h]))
        mine[h].start()
    mine_left = pltpu.make_async_copy(left_ref, lbuf.at[me], own.at[chunks])
    mine_left.start()

    rwide[...] = jnp.zeros_like(rwide)
    channels = width * width
    for start in range(0, channels, LANES):
        chosen = swap_matrix(width, width, start, LANES, channels)
        block = jnp.dot(chosen, weight_ref[...], preferred_element_type=jnp.float32)
        wturn[:, start : start + LANES] = block.T.astype(jnp.bfloat16)
    swap = swap_matrix(TILE, part, 0, TILE * part, TILE * part)

    forwards = []
    for k in range(1, hops):
        slot = lax.rem(me + n - GROUP * k, n)
        lcopy(left_ref, slot, mates[0], lsend.at[k]).wait_recv()
        for j, mate in enumerate(mates):
            forward = lcopy(lbuf.at[slot], slot, mate, fsend.at[k, j])
            forward.start()
            forwards.append(forward)
    for k in range(hops):
        for j, mate in enumerate(mates):
            slot = lax.rem(mate + n - GROUP * k, n)
            lcopy(left_ref, slot, mate, fsend.at[k, j]).wait_recv()
    mine_left.wait()
    per = TILE // local
    blocks = []
    for group in range(seqs // TILE):
        parts = [lbuf[group * per + p] for p in range(per)]
        if per > 1:
            parts = [piece.astype(jnp.float32) for piece in parts]
            blocks.append(jnp.concatenate(parts, axis=0).astype(jnp.bfloat16))
        else:
            blocks.append(parts[0])
    lturn[...] = jnp.concatenate(blocks, axis=0).T

    def turn(h, start, block):
        turned = lax.dot_general(
            swap, block, (((1,), (1,)), ((), ())), preferred_element_type=jnp.float32
        ).astype(jnp.bfloat16)
        for e in range(part):
            at = (h * part + e) * LANES
            rwide[pl.ds(start, TILE), at : at + cols] = turned[e * TILE : (e + 1) * TILE]

    def arrive(h):
        def one(k, carry):
            slot = lax.rem(me + n - k, n)
            pltpu.make_async_remote_copy(
                src_ref=right_ref.at[h, pl.ds(0, cols)],
                dst_ref=rbuf.at[h, slot],
                send_sem=rsend.at[h, k],
                recv_sem=rrecv.at[h, slot],
                device_id={"col": slot},
                device_id_type=MESH,
            ).wait_recv()
            if per == 1:
                turn(h, pl.multiple_of(slot * TILE, TILE), rbuf[h, slot])
            return carry

        mine[h].wait()
        if per == 1:
            turn(h, pl.multiple_of(me * TILE, TILE), rbuf[h, me])
        lax.fori_loop(1, n, one, 0)
        if per > 1:
            for group in range(seqs // TILE):
                parts = [rbuf[h, group * per + p] for p in range(per)]
                turn(h, group * TILE, jnp.concatenate(parts, axis=1))

    count = flat.shape[0] * 2

    def multiply(base, h):
        def outer(step, carry):
            lanes = pl.ds(pl.multiple_of(step * 2 * LANES, 2 * LANES), 2 * LANES)
            product = jnp.dot(
                lturn[base * width : (base + count) * width, :],
                rwide[:, lanes],
                preferred_element_type=jnp.float32,
            ).astype(jnp.bfloat16)
            for side_e in range(2):
                at = pl.ds(pl.multiple_of((step * 2 + side_e) * width, width), width)
                for i in range(count):
                    side = (i % 2) * LANES
                    flat[i // 2, at, side : side + LANES] = product[
                        i * width : (i + 1) * width, side_e * LANES : (side_e + 1) * LANES
                    ]
            return carry

        lax.fori_loop(h * part // 2, (h + 1) * part // 2, outer, 0)

    deep = part * width
    early = rows == count and chunks > 1

    def project_early(step, carry):
        partial[step] = jnp.dot(
            wturn[:, : channels - deep],
            flat[step, : channels - deep],
            preferred_element_type=jnp.float32,
        )
        return carry

    for h in range(chunks):
        arrive(h)
        if rows == count:
            multiply(0, h)
        if early and h == chunks - 2:
            lax.fori_loop(0, count // 2, project_early, 0)

    skip = channels - deep if early else 0
    for base in range(0, rows, count):
        if rows != count:
            for h in range(chunks):
                multiply(base, h)

        def project(step, carry):
            update = jnp.dot(
                wturn[:, skip:], flat[step, skip:], preferred_element_type=jnp.float32
            )
            if early:
                update = update + partial[step]
            update = update.T * (1.0 / seqs) + bias_ref[...]
            update = update.astype(out_ref.dtype)
            out_ref[base + 2 * step] = update[:cols]
            out_ref[base + 2 * step + 1] = update[LANES : LANES + cols]
            return carry

        lax.fori_loop(0, count // 2, project, 0)

    for copy in sends + forwards:
        copy.wait_send()


def on_device(n, left, right, out_weight, out_bias):
    local, rows, width = left.shape
    cols = right.shape[1] // n
    pair = out_weight.shape[1]
    seqs = local * n
    chunks = 2 if local * width % (4 * LANES) == 0 else 1
    turned = flip(jnp.transpose(right, (0, 2, 1)), chunks)
    rows_step = min(rows, 32)
    vmem = pl.BlockSpec(memory_space=pltpu.VMEM)
    dma = pltpu.SemaphoreType.DMA
    return pl.pallas_call(
        functools.partial(kernel, n, width, cols, rows, chunks),
        out_shape=jax.ShapeDtypeStruct((rows, cols, pair), jnp.bfloat16),
        in_specs=[vmem] * 4,
        out_specs=vmem,
        scratch_shapes=[
            pltpu.VMEM((chunks, n, cols, local * width // chunks), jnp.bfloat16),
            pltpu.VMEM((n, local, rows * width), jnp.bfloat16),
            pltpu.VMEM((seqs, width * LANES), jnp.bfloat16),
            pltpu.VMEM((rows * width, seqs), jnp.bfloat16),
            pltpu.VMEM((pair, width * width), jnp.bfloat16),
            pltpu.VMEM((rows_step // 2, width * width, 2 * LANES), jnp.bfloat16),
            pltpu.VMEM((rows_step // 2, pair, 2 * LANES), jnp.float32),
            dma((chunks, n)), dma((chunks, n)),
            dma((n // GROUP,)), dma((n,)), dma((n // GROUP, GROUP)), dma((chunks + 1,)),
        ],
        compiler_params=pltpu.CompilerParams(
            collective_id=0, has_side_effects=True, vmem_limit_bytes=60 * 1024 * 1024
        ),
    )(turned, left.reshape(local, rows * width), out_weight, out_bias.reshape(1, pair))


def solution(mesh):
    return jax.shard_map(
        functools.partial(on_device, mesh.shape["col"]),
        mesh=mesh,
        in_specs=(P("col", "groups", None), P("col", "groups", None), P(), P()),
        out_specs=P("groups", "col", None),
        check_vma=False,
    )
```

```python
import functools

import jax
import jax.numpy as jnp
from jax import lax
from jax.experimental import pallas as pl
from jax.experimental.pallas import tpu as pltpu
from jax.sharding import PartitionSpec as P

MESH = pl.DeviceIdType.MESH
LANES = 128
TILE = 16
GROUP = 4


def flip(x_ref, o_ref, h):
    chunks, columns, lanes = o_ref.shape
    part = x_ref.shape[1] // chunks
    step = 2 * LANES
    for start in range(0, columns, step):
        piece = x_ref[:, h * part : (h + 1) * part, start : start + step]
        o_ref[h, start : start + step] = piece.reshape(lanes, step).T


def swap_matrix(first, minor, start, rows, columns):
    row = lax.broadcasted_iota(jnp.int32, (rows, columns), 0) + start
    column = lax.broadcasted_iota(jnp.int32, (rows, columns), 1)
    shift = first.bit_length() - 1
    wanted = (row & (first - 1)) * minor + (row >> shift)
    return jnp.where(column == wanted, 1.0, 0.0).astype(jnp.bfloat16)


def kernel(
    n, width, cols, rows, chunks, given_ref, left_ref, weight_ref, bias_ref, out_ref,
    right_ref, rbuf, lbuf, rwide, lturn, wturn, flat, partial,
    rsend, rrecv, lsend, lrecv, fsend, own,
):
    me = lax.axis_index("col")
    place = lax.rem(me, GROUP)
    mates = [me - place + lax.rem(place + j, GROUP) for j in range(1, GROUP)]
    hops = n // GROUP
    local = left_ref.shape[0]
    seqs = n * local
    part = width // chunks

    def rcopy(h, k):
        to = lax.rem(me + k, n)
        start = pl.multiple_of(to * cols, TILE)
        return pltpu.make_async_remote_copy(
            src_ref=right_ref.at[h, pl.ds(start, cols)],
            dst_ref=rbuf.at[h, me],
            send_sem=rsend.at[h, k],
            recv_sem=rrecv.at[h, me],
            device_id={"col": to},
            device_id_type=MESH,
        )

    def lcopy(src, slot, to, send):
        return pltpu.make_async_remote_copy(
            src_ref=src,
            dst_ref=lbuf.at[slot],
            send_sem=send,
            recv_sem=lrecv.at[slot],
            device_id={"col": to},
            device_id_type=MESH,
        )

    barrier = pltpu.get_barrier_semaphore()
    for k in range(1, n):
        pl.semaphore_signal(
            barrier, inc=1, device_id={"col": lax.rem(me + k, n)}, device_id_type=MESH
        )
    flip(given_ref, right_ref, 0)
    pl.semaphore_wait(barrier, n - 1)

    sends = []
    for k in range(1, hops):
        sends.append(lcopy(left_ref, me, lax.rem(me + GROUP * k, n), lsend.at[k]))
    for j, mate in enumerate(mates):
        sends.append(lcopy(left_ref, me, mate, fsend.at[0, j]))
    for k in range(1, n):
        sends.append(rcopy(0, k))
    for copy in sends:
        copy.start()
    for h in range(1, chunks):
        flip(given_ref, right_ref, h)
    mine_left = pltpu.make_async_copy(left_ref, lbuf.at[me], own.at[chunks])
    mine_left.start()

    rwide[...] = jnp.zeros_like(rwide)
    channels = width * width
    for start in range(0, channels, LANES):
        chosen = swap_matrix(width, width, start, LANES, channels)
        block = jnp.dot(chosen, weight_ref[...], preferred_element_type=jnp.float32)
        wturn[:, start : start + LANES] = block.T.astype(jnp.bfloat16)
    for h in range(1, chunks):
        later = [rcopy(h, k) for k in range(1, n)]
        for copy in later:
            copy.start()
        sends += later
    mine = []
    for h in range(chunks):
        block = right_ref.at[h, pl.ds(pl.multiple_of(me * cols, TILE), cols)]
        mine.append(pltpu.make_async_copy(block, rbuf.at[h, me], own.at[h]))
        mine[h].start()
    swap = swap_matrix(TILE, part, 0, TILE * part, TILE * part)

    forwards = []
    for k in range(1, hops):
        slot = lax.rem(me + n - GROUP * k, n)
        lcopy(left_ref, slot, mates[0], lsend.at[k]).wait_recv()
        for j, mate in enumerate(mates):
            forward = lcopy(lbuf.at[slot], slot, mate, fsend.at[k, j])
            forward.start()
            forwards.append(forward)
    for k in range(hops):
        for j, mate in enumerate(mates):
            slot = lax.rem(mate + n - GROUP * k, n)
            lcopy(left_ref, slot, mate, fsend.at[k, j]).wait_recv()
    mine_left.wait()
    per = TILE // local
    blocks = []
    for group in range(seqs // TILE):
        parts = [lbuf[group * per + p] for p in range(per)]
        if per > 1:
            parts = [piece.astype(jnp.float32) for piece in parts]
            blocks.append(jnp.concatenate(parts, axis=0).astype(jnp.bfloat16))
        else:
            blocks.append(parts[0])
    lturn[...] = jnp.concatenate(blocks, axis=0).T

    def turn(h, start, block):
        turned = lax.dot_general(
            swap, block, (((1,), (1,)), ((), ())), preferred_element_type=jnp.float32
        ).astype(jnp.bfloat16)
        for e in range(part):
            at = (h * part + e) * LANES
            rwide[pl.ds(start, TILE), at : at + cols] = turned[e * TILE : (e + 1) * TILE]

    def arrive(h):
        def one(k, carry):
            slot = lax.rem(me + n - k, n)
            pltpu.make_async_remote_copy(
                src_ref=right_ref.at[h, pl.ds(0, cols)],
                dst_ref=rbuf.at[h, slot],
                send_sem=rsend.at[h, k],
                recv_sem=rrecv.at[h, slot],
                device_id={"col": slot},
                device_id_type=MESH,
            ).wait_recv()
            if per == 1:
                turn(h, pl.multiple_of(slot * TILE, TILE), rbuf[h, slot])
            return carry

        mine[h].wait()
        if per == 1:
            turn(h, pl.multiple_of(me * TILE, TILE), rbuf[h, me])
        lax.fori_loop(1, n, one, 0)
        if per > 1:
            for group in range(seqs // TILE):
                parts = [rbuf[h, group * per + p] for p in range(per)]
                turn(h, group * TILE, jnp.concatenate(parts, axis=1))

    count = flat.shape[0] * 2

    def multiply(base, h):
        def outer(step, carry):
            lanes = pl.ds(pl.multiple_of(step * 2 * LANES, 2 * LANES), 2 * LANES)
            product = jnp.dot(
                lturn[base * width : (base + count) * width, :],
                rwide[:, lanes],
                preferred_element_type=jnp.float32,
            ).astype(jnp.bfloat16)
            for side_e in range(2):
                at = pl.ds(pl.multiple_of((step * 2 + side_e) * width, width), width)
                for i in range(count):
                    side = (i % 2) * LANES
                    flat[i // 2, at, side : side + LANES] = product[
                        i * width : (i + 1) * width, side_e * LANES : (side_e + 1) * LANES
                    ]
            return carry

        lax.fori_loop(h * part // 2, (h + 1) * part // 2, outer, 0)

    deep = part * width
    early = rows == count and chunks > 1

    def project_early(step, carry):
        partial[step] = jnp.dot(
            wturn[:, : channels - deep],
            flat[step, : channels - deep],
            preferred_element_type=jnp.float32,
        )
        return carry

    for h in range(chunks):
        arrive(h)
        if rows == count:
            multiply(0, h)
        if early and h == chunks - 2:
            lax.fori_loop(0, count // 2, project_early, 0)

    skip = channels - deep if early else 0
    for base in range(0, rows, count):
        if rows != count:
            for h in range(chunks):
                multiply(base, h)

        def project(step, carry):
            update = jnp.dot(
                wturn[:, skip:], flat[step, skip:], preferred_element_type=jnp.float32
            )
            if early:
                update = update + partial[step]
            update = update.T * (1.0 / seqs) + bias_ref[...]
            update = update.astype(out_ref.dtype)
            out_ref[base + 2 * step] = update[:cols]
            out_ref[base + 2 * step + 1] = update[LANES : LANES + cols]
            return carry

        lax.fori_loop(0, count // 2, project, 0)

    for copy in sends + forwards:
        copy.wait_send()


def on_device(n, left, right, out_weight, out_bias):
    local, rows, width = left.shape
    cols = right.shape[1] // n
    pair = out_weight.shape[1]
    seqs = local * n
    chunks = 2 if local * width % (4 * LANES) == 0 else 1
    rows_step = min(rows, 32)
    vmem = pl.BlockSpec(memory_space=pltpu.VMEM)
    dma = pltpu.SemaphoreType.DMA
    return pl.pallas_call(
        functools.partial(kernel, n, width, cols, rows, chunks),
        out_shape=jax.ShapeDtypeStruct((rows, cols, pair), jnp.bfloat16),
        in_specs=[vmem] * 4,
        out_specs=vmem,
        scratch_shapes=[
            pltpu.VMEM((chunks, right.shape[1], local * width // chunks), jnp.bfloat16),
            pltpu.VMEM((chunks, n, cols, local * width // chunks), jnp.bfloat16),
            pltpu.VMEM((n, local, rows * width), jnp.bfloat16),
            pltpu.VMEM((seqs, width * LANES), jnp.bfloat16),
            pltpu.VMEM((rows * width, seqs), jnp.bfloat16),
            pltpu.VMEM((pair, width * width), jnp.bfloat16),
            pltpu.VMEM((rows_step // 2, width * width, 2 * LANES), jnp.bfloat16),
            pltpu.VMEM((rows_step // 2, pair, 2 * LANES), jnp.float32),
            dma((chunks, n)), dma((chunks, n)),
            dma((n // GROUP,)), dma((n,)), dma((n // GROUP, GROUP)), dma((chunks + 1,)),
        ],
        compiler_params=pltpu.CompilerParams(
            collective_id=0, has_side_effects=True, vmem_limit_bytes=60 * 1024 * 1024
        ),
    )(jnp.transpose(right, (0, 2, 1)), left.reshape(local, rows * width), out_weight, out_bias.reshape(1, pair))


def solution(mesh):
    return jax.shard_map(
        functools.partial(on_device, mesh.shape["col"]),
        mesh=mesh,
        in_specs=(P("col", "groups", None), P("col", "groups", None), P(), P()),
        out_specs=P("groups", "col", None),
        check_vma=False,
    )
```
